32 devices in a mesh: segment: 8 (over z, x), dp: 4 (over y, core).
Axes of the slice: x: 2, y: 2, z: 4, core: 2. Of those that a mesh axis runs over, the one named last changes fastest.
Arguments:
- src_embed: bfloat16 [16, 128, 2048], P('dp', None, 'segment'), parts along dimension 0, may hold values from -6 to 6
- tgt_embed: bfloat16 [16, 128, 2048], P('dp', None, 'segment'), parts along dimension 0, may hold values from -6 to 6
- src_lengths: int32 [16], P('dp'), parts along dimension 0, may hold values from 32 to 128
- tgt_lengths: int32 [16], P('dp'), parts along dimension 0, may hold values from 32 to 128
- attn_in: bfloat16 [8, 2048, 3072], P('segment'), may hold values from -0.125 to 0.125
- attn_out: bfloat16 [8, 1024, 2048], P('segment'), may hold values from -0.375 to 0.375
- norm_gain: float32 [4, 2048], replicated, may hold values from 0.25 to 1.75
- final_gain: float32 [2048], replicated, may hold values from 0.25 to 1.75
Outputs:
- decoded: bfloat16 [16, 128, 2048], P('dp', None, 'segment'), parts along dimension 0
The draws below stay inside these ranges and needn't reach their ends.
There are 4 independent parts, one for each index of `dp`. The reference program is written for one: setup_inputs(seed, part) draws one part's arguments, and reference() takes and returns one part's arrays. A program takes and returns all parts, laid end to end along the dimension named above; an argument that names none is the same for every part. Nothing has to cross between parts.
Inputs may be any that keep to these rules, and one draw needn't show every extreme that they name: `src_lengths`: keys at positions below a sequence's length are its real tokens. `tgt_lengths`: keys at positions below a sequence's length are its real tokens.
All inputs are finite; a program needn't handle non-finite values.
Results may differ from the reference program's by a relative error of at most 0.015.
Values may be sent and summed in bfloat16 or wider, within the bound.
A program may use at most 64 MiB of HBM per device.

```python
import jax
import jax.numpy as jnp
from jax import lax

D = 2048
HEAD = 64
MB = 4
S = 128
GROUP = 2
INNER = 2048
N_SEGMENT = 8


def place_ends(drawn, key, smallest, top_value):
    shape = drawn.shape
    index_at = [jax.random.randint(jax.random.fold_in(key, axis), (), 0, shape[axis]) for axis in range(len(shape))]
    drawn = drawn.at[tuple(index_at)].set(smallest)
    longest = shape.index(max(shape))
    index_at[longest] = (index_at[longest] + 1) % shape[longest]
    return drawn.at[tuple(index_at)].set(top_value)


def block_levels(stream_key, extent, cuts, low, top_value):
    def one(axis_at, blocks):
        steps = jax.random.uniform(jax.random.fold_in(jax.random.fold_in(stream_key, 6), axis_at), (blocks,), jnp.float32, low / len(cuts), top_value / len(cuts))
        return jnp.repeat(jnp.exp(steps), extent[axis_at] // blocks).reshape((-1,) + (1,) * (len(extent) - axis_at - 1))

    gain = one(*cuts[0])
    for cut in cuts[1:]:
        gain = gain * one(*cut)
    return gain


def centred(own_key, shape, deviation, most, cuts=(), kind=jnp.bfloat16):
    array = jax.random.normal(own_key, shape, jnp.float32) * deviation
    if len(cuts) > 0:
        array = block_levels(own_key, shape, cuts, -0.22, 0.18) * array
    return jnp.clip(array, min=-most, max=most).astype(kind)


def setup_inputs(seed: int = 0, part: int = 0) -> dict:
    key_list = jax.random.split(jax.random.key(seed), 9)
    part_keys = jax.random.split(jax.random.fold_in(key_list[8], part), 9)
    return {
        "src_embed": centred(part_keys[0], (MB, S, D), 1.0, 6.0, ((2, 8),)),
        "tgt_embed": centred(part_keys[1], (MB, S, D), 1.0, 6.0, ((2, 8),)),
        "src_lengths": place_ends(jax.random.randint(part_keys[2], (MB,), S // 4, S + 1), jax.random.fold_in(part_keys[2], 1), S // 4, S).astype(jnp.int32),
        "tgt_lengths": place_ends(jax.random.randint(part_keys[3], (MB,), S // 4, S + 1), jax.random.fold_in(part_keys[3], 1), S // 4, S).astype(jnp.int32),
        "attn_in": centred(key_list[4], (N_SEGMENT, D, 3 * INNER // GROUP), D ** -0.5, 0.125, ((0, 8),)),
        "attn_out": centred(key_list[5], (N_SEGMENT, INNER // GROUP, D), (INNER // 8) ** -0.5, 0.375, ((0, 8),)),
        "norm_gain": jnp.clip(1.0 + 0.15 * jax.random.normal(key_list[6], (4, D), jnp.float32), 0.25, 1.75),
        "final_gain": jnp.clip(1.0 + 0.15 * jax.random.normal(key_list[7], (D,), jnp.float32), 0.25, 1.75),
    }


epsilon = 1e-06
score_scale = 0.125

def rms_scale(values, gain_vector):
    return values * lax.rsqrt(lax.optimization_barrier(jnp.mean(values * values, axis=-1, keepdims=True)) + epsilon) * gain_vector

def attention(queries, key_rows, values, allowed):
    head_count = queries.shape[1] // HEAD
    shaped_q = queries.reshape(queries.shape[0], head_count, HEAD).astype(jnp.float32)
    shaped_k = key_rows.reshape(key_rows.shape[0], head_count, HEAD).astype(jnp.float32)
    shaped_v = values.reshape(values.shape[0], head_count, HEAD).astype(jnp.float32)
    scores = jnp.einsum('qhd,khd->hqk', shaped_q, shaped_k) * score_scale
    scores = jnp.where(allowed[None], scores, -1000000000.0)
    weights = jax.nn.softmax(scores, axis=-1).astype(jnp.bfloat16)
    mixture = jnp.einsum('hqk,khd->qhd', weights.astype(jnp.float32), shaped_v)
    return mixture.reshape(queries.shape[0], -1).astype(jnp.bfloat16)

def sublayer(inputs, memory, attn_in, attn_out, norm_gain, layer_slot, group_size, allowed):
    normed = rms_scale(inputs.astype(jnp.float32), norm_gain[layer_slot]).astype(jnp.bfloat16)
    source = normed if memory is None else memory
    summed = jnp.zeros(inputs.shape, jnp.float32)
    for member in range(group_size):
        weight_slot = layer_slot * group_size + member
        in_weight = attn_in[weight_slot]
        out_weight = attn_out[weight_slot]
        head_cols = out_weight.shape[0]
        queries = jnp.dot(normed, in_weight[:, :head_cols], preferred_element_type=jnp.float32).astype(jnp.bfloat16)
        key_value = jnp.dot(source, in_weight[:, head_cols:], preferred_element_type=jnp.float32).astype(jnp.bfloat16)
        mixture = attention(queries, key_value[:, :head_cols], key_value[:, head_cols:], allowed)
        summed = summed + jnp.dot(mixture, out_weight, preferred_element_type=jnp.float32)
    return (inputs.astype(jnp.float32) + summed).astype(jnp.bfloat16)

def reference(src_embed, tgt_embed, src_lengths, tgt_lengths, attn_in, attn_out, norm_gain, final_gain):
    group_size = N_SEGMENT // 4
    positions = jnp.arange(S, dtype=jnp.int32)
    causal = positions[None, :] <= positions[:, None]
    results = []
    for batch_slot in range(MB):
        source_ok = jnp.broadcast_to(positions[None, :] < src_lengths[batch_slot], (S, S))
        target_ok = (positions[None, :] < tgt_lengths[batch_slot]) & causal
        encoded = src_embed[batch_slot]
        for layer_slot in range(2):
            encoded = sublayer(encoded, None, attn_in, attn_out, norm_gain, layer_slot, group_size, source_ok)
        memory = rms_scale(encoded.astype(jnp.float32), final_gain).astype(jnp.bfloat16)
        decoded = sublayer(tgt_embed[batch_slot], memory, attn_in, attn_out, norm_gain, 2, group_size, source_ok)
        decoded = sublayer(decoded, None, attn_in, attn_out, norm_gain, 3, group_size, target_ok)
        results.append(decoded)
    return jnp.stack(results)
```

```python
import functools

import jax
import jax.numpy as jnp
from jax import lax
from jax.experimental import pallas as pl
from jax.experimental.pallas import tpu as pltpu
from jax.sharding import PartitionSpec as P

HEAD = 64
LAYERS = 4
MESH = pl.DeviceIdType.MESH
SENT = 2
PLAN = (
    ("turn", 0),
    ("combine", 0),
    ("combine", 1),
    ("combine", 2),
    ("combine", 3),
    ("stage", 0),
    ("stage", 1),
    ("stage", 2),
    ("stage", 3),
)
epsilon = 1e-06
score_scale = 0.125


def kernel(
    segs,
    src_len,
    tgt_len,
    src,
    tgt,
    w_in,
    w_out,
    gains,
    final_gain,
    out,
    win,
    wout,
    act,
    nrm,
    qkv,
    mix,
    own,
    ps,
    pr,
    fw,
    w_sem,
    act_sem,
    in_send,
    p_send,
    p_recv,
    f_send,
    o_recv,
    go,
    side,
    side_send,
    side_recv,
    on_send,
    r_send,
    t_send,
    turn,
):
    group = segs // LAYERS
    batches, seq, cw = src.shape
    width = segs * cw
    hc = wout.shape[0]
    me = lax.axis_index("segment")
    section = me // group
    member = me % group
    is_cross = section == 2
    is_last = section == LAYERS - 1
    q_src = jnp.where(is_cross, 1, 0)

    win_copy = pltpu.make_async_copy(w_in, win, w_sem.at[0])
    wout_copy = pltpu.make_async_copy(w_out, wout, w_sem.at[1])
    win_copy.start()
    wout_copy.start()

    barrier = pltpu.get_barrier_semaphore()
    for step in range(1, segs):
        pl.semaphore_signal(
            barrier,
            inc=1,
            device_id={"segment": lax.rem(me + step, segs)},
            device_id_type=MESH,
        )
    lane_at = lax.axis_index("dp")
    leads = lane_at % 2 == 1
    mate = lane_at + 1 - 2 * (lane_at % 2)
    pl.semaphore_signal(
        barrier, inc=1, device_id={"dp": mate}, device_id_type=MESH
    )
    pl.semaphore_wait(barrier, segs)

    def remote(source, dest, send, recv, target):
        return pltpu.make_async_remote_copy(
            src_ref=source,
            dst_ref=dest,
            send_sem=send,
            recv_sem=recv,
            device_id={"segment": target},
            device_id_type=MESH,
        )

    def input_copy(kind, m, j):
        ref = src if kind == 0 else tgt
        target = 2 * kind * group + j
        return remote(
            ref.at[m],
            act.at[kind, m, me],
            in_send.at[kind, m, j],
            act_sem.at[kind, m, me],
            target,
        )

    def sends(kind, m, j):
        if kind == 1:
            return jnp.logical_or(j == member, is_cross)
        return jnp.logical_or(j == member, jnp.logical_and(section == 0, m > 0))

    def send_inputs(kind, m):
        ref = src if kind == 0 else tgt
        for j in range(group):
            target = 2 * kind * group + j

            @pl.when(jnp.logical_and(sends(kind, m, j), me != target))
            def _():
                input_copy(kind, m, j).start()

            @pl.when(me == target)
            def _():
                pltpu.make_async_copy(
                    ref.at[m], act.at[kind, m, me], act_sem.at[kind, m, me]
                ).start()

    def beside(g):
        return section * group + lax.rem(member + g, group)

    def side_copy(m, g):
        return remote(
            src.at[m],
            side.at[m - 1, g - 1],
            side_send.at[m - 1, g - 1],
            side_recv.at[m - 1, g - 1],
            beside(g),
        )

    def side_on(m, g):
        source = beside(group - g)
        return remote(
            side.at[m - 1, g - 1],
            act.at[0, m, source],
            on_send.at[m - 1, g - 1],
            act_sem.at[0, m, source],
            member,
        )

    def relay(m, c, g):
        return remote(
            act.at[0, m, c],
            act.at[0, m, c],
            r_send.at[m, g - 1, c],
            act_sem.at[0, m, c],
            beside(g),
        )

    send_inputs(0, 0)

    @pl.when(section > 0)
    def _():
        for m in range(1, batches):
            for g in range(1, group):
                side_copy(m, g).start()

    @pl.when(section <= 2)
    def _():
        for m in range(batches):
            send_inputs(1, m)

    def act_wait(kind, m, c):
        pltpu.make_async_copy(
            act.at[kind, m, c], act.at[kind, m, c], act_sem.at[kind, m, c]
        ).wait()

    def pass_on(m, order):
        for c in order:

            @pl.when(c % group == member)
            def _(c=c):
                act_wait(0, m, c)
                for g in range(1, group):
                    relay(m, c, g).start()

    def release(k, first):
        for c in range(first * group, segs):

            @pl.when(me != c)
            def _(c=c):
                pl.semaphore_signal(
                    go.at[k - 1],
                    inc=1,
                    device_id={"segment": c},
                    device_id_type=MESH,
                )

    @pl.when(section == 0)
    def _():
        pass_on(0, tuple(range(group)) + tuple(range(segs - 1, 2 * group - 1, -1)))
        release(1, 0)
        pass_on(0, range(group, 2 * group))

    def cross_relay(m, c, g):
        return remote(
            act.at[1, m, c],
            act.at[1, m, c],
            t_send.at[m, g - 1, c],
            act_sem.at[1, m, c],
            beside(g),
        )

    def spread_targets(planes):
        for m in range(batches):
            for p in planes:
                for c in range(p * group, (p + 1) * group):

                    @pl.when(jnp.logical_and(is_cross, c % group == member))
                    def _(m=m, c=c, p=p):
                        act_wait(1, m, c)
                        if p != 2:
                            for g in range(1, group):
                                cross_relay(m, c, g).start()

    pl.semaphore_wait(go.at[0], jnp.where(section == 0, group - 1, group))
    for m in range(1, batches):
        if m > 1:
            first = 1 if m == 2 else 2

            @pl.when(section >= first)
            def _(m=m):
                pl.semaphore_wait(go.at[m - 1], group)

        send_inputs(0, m)

        @pl.when(section > 0)
        def _(m=m):
            for g in range(1, group):
                side_copy(m, g).wait_recv()
                side_on(m, g).start()

        if m == 1:

            @pl.when(section > 2)
            def _():
                for k in range(batches):
                    send_inputs(1, k)

            spread_targets((2, 1, 0))

        if m == min(2, batches - 1):
            spread_targets((3,))

    def normalize(kind, m, gain_row):
        total = jnp.zeros((seq, cw), jnp.float32)
        for c in range(segs):
            v = act[kind, m, c].astype(jnp.float32)
            total = total + v * v
        mean = jnp.sum(total, axis=-1, keepdims=True) * (1.0 / width)
        scale = lax.rsqrt(mean + epsilon)
        for c in range(segs):
            v = act[kind, m, c].astype(jnp.float32)
            g = gain_row(c)
            nrm[kind, :, c * cw : (c + 1) * cw] = (v * scale * g).astype(jnp.bfloat16)

    def key_gain(c):
        cols = slice(c * cw, (c + 1) * cw)
        picked = jnp.where(is_cross, final_gain[:, cols], gains[0:1, cols])
        for p in (1, 3):
            picked = jnp.where(section == p, gains[p : p + 1, cols], picked)
        return picked

    def query_gain(c):
        return gains[2:3, c * cw : (c + 1) * cw]

    def part_copy(m, c, g):
        target = section * group + lax.rem(member + g, group)
        return remote(
            ps.at[m, c],
            pr.at[m, g - 1, c],
            p_send.at[m, g - 1, c],
            p_recv.at[m, g - 1, c],
            target,
        )

    def whole_from(p, m):
        inner = m > 0
        return jnp.logical_and(p < LAYERS - 1, inner)

    def whole(m):
        return whole_from(section, m)

    def halved(m):
        later = jnp.logical_and(section > 0, jnp.logical_not(whole_from(section - 1, m)))
        return jnp.logical_or(m == 0, later)

    def part_needed(m, c, g):
        goal = lax.rem(member + g, group)
        return jnp.logical_or(whole(m), lax.rem(c, group) == goal)

    def keeps(m, c):
        return jnp.logical_or(whole(m), lax.rem(c, group) == member)

    def next_copy(m, c):
        return remote(
            fw.at[m, c], act.at[0, m, c], f_send.at[m, c], act_sem.at[0, m, c], me + group
        )

    def out_copy(m, c):
        return remote(fw.at[m, c], out.at[m], f_send.at[m, c], o_recv.at[m], c)

    tile = min(512, hc)
    kv_tiles = 2 * hc // tile
    q_tiles = hc // tile

    def prepare(m):
        @pl.when(is_cross)
        def _():
            for c in range(segs):

                @pl.when(c % group != member)
                def _(c=c):
                    act_wait(1, m, c)

            normalize(1, m, query_gain)

        @pl.when(jnp.logical_and(section > 0, m == 0))
        def _():
            pass_on(0, range(segs))

        for c in range(segs):

            @pl.when(jnp.logical_not(jnp.logical_and(halved(m), c % group == member)))
            def _(c=c):
                act_wait(0, m, c)

        normalize(0, m, key_gain)

        @pl.when(m == 0)
        def _():
            win_copy.wait()


    def project(t, carry):
        kind = jnp.where(t < q_tiles, q_src, 0)
        cols = pl.ds(pl.multiple_of(t * tile, tile), tile)
        qkv[:, cols] = jnp.dot(
            nrm[kind], win[:, cols], preferred_element_type=jnp.float32
        ).astype(jnp.bfloat16)
        return carry

    def attend(m):
        length = jnp.where(is_last, tgt_len[m], src_len[m])
        keys = lax.broadcasted_iota(jnp.int32, (2 * seq, seq), 1)
        rows = lax.broadcasted_iota(jnp.int32, (2 * seq, seq), 0)
        rows = jnp.where(rows >= seq, rows - seq, rows)
        bound = jnp.where(is_last, rows, seq)
        allowed = (keys < length) & (keys <= bound)
        lane = lax.broadcasted_iota(jnp.int32, (seq, 2 * HEAD), 1)
        low = lane < HEAD
        for h in range(hc // (2 * HEAD)):
            at = h * 2 * HEAD
            q2 = qkv[:, at : at + 2 * HEAD]
            k2 = qkv[:, hc + at : hc + at + 2 * HEAD]
            v2 = qkv[:, 2 * hc + at : 2 * hc + at + 2 * HEAD]
            zero = jnp.zeros_like(q2)
            both = jnp.concatenate(
                [jnp.where(low, q2, zero), jnp.where(low, zero, q2)], axis=0
            )
            scores = (
                lax.dot_general(
                    both,
                    k2,
                    (((1,), (1,)), ((), ())),
                    preferred_element_type=jnp.float32,
                )
                * score_scale
            )
            scores = jnp.where(allowed, scores, -1000000000.0)
            top = jnp.max(scores, axis=-1, keepdims=True)
            e = jnp.exp(scores - top)
            weights = (e / jnp.sum(e, axis=-1, keepdims=True)).astype(jnp.bfloat16)
            o = jnp.dot(weights, v2, preferred_element_type=jnp.float32)
            mix[:, at : at + 2 * HEAD] = jnp.where(low, o[:seq], o[seq:]).astype(
                jnp.bfloat16
            )

    def send_parts(m):
        @pl.when(m == 0)
        def _():
            wout_copy.wait()

        def emit(c, carry):
            cols = pl.ds(pl.multiple_of(c * cw, cw), cw)
            part = jnp.dot(mix[...], wout[:, cols], preferred_element_type=jnp.float32)
            own[c] = part
            ps[m, c] = part.astype(jnp.bfloat16)

            @pl.when(jnp.logical_and(c == 0, jnp.logical_or(m > 0, jnp.logical_not(leads))))
            def _():
                pl.semaphore_wait(turn, 1)

            for g in range(1, group):

                @pl.when(part_needed(m, c, g))
                def _():
                    part_copy(m, c, g).start()

            return carry

        lax.fori_loop(0, segs, emit, 0, unroll=True)

    def hand_over(m):
        for c in range(SENT):
            for g in range(1, group):

                @pl.when(part_needed(m, c, g))
                def _(c=c, g=g):
                    part_copy(m, c, g).wait_send()

        @pl.when(jnp.logical_or(m < batches - 1, leads))
        def _():
            pl.semaphore_signal(
                turn, inc=1, device_id={"dp": mate}, device_id_type=MESH
            )

    def combine(m, c):
        @pl.when(keeps(m, c))
        def _():
            total = own[c] + act[q_src, m, c].astype(jnp.float32)
            for g in range(1, group):
                part_copy(m, c, g).wait_recv()
                total = total + pr[m, g - 1, c].astype(jnp.float32)
            fw[m, c] = total.astype(jnp.bfloat16)

            @pl.when(section < LAYERS - 1)
            def _():
                next_copy(m, c).start()

            @pl.when(jnp.logical_and(is_last, me != c))
            def _():
                out_copy(m, c).start()

            @pl.when(jnp.logical_and(is_last, me == c))
            def _():
                pltpu.make_async_copy(fw.at[m, c], out.at[m], o_recv.at[m]).start()

    half = (q_tiles + kv_tiles) // 2
    stages = (
        prepare,
        lambda m: lax.fori_loop(0, half, project, 0, unroll=True),
        lambda m: lax.fori_loop(half, q_tiles + kv_tiles, project, 0, unroll=True),
        attend,
    )

    def batch_step(t, carry):
        m = t - 1
        active = t < batches

        @pl.when(t > 0)
        def _():
            send_parts(m)

        for k in range(2, batches):

            @pl.when(jnp.logical_and(section == 0, t == k - 1))
            def _(k=k):
                release(k, 1 if k == 2 else 2)

        for op, i in PLAN:
            if op == "combine":

                @pl.when(t > 0)
                def _(i=i):
                    for c in range(i * group, (i + 1) * group):
                        combine(m, c)

            elif op == "turn":

                @pl.when(t > 0)
                def _():
                    hand_over(m)

            elif op == "relay":
                due = jnp.logical_and(t > 0, jnp.logical_and(active, section > 0))

                @pl.when(jnp.logical_and(due, halved(jnp.minimum(t, batches - 1))))
                def _(i=i):
                    pass_on(t, range(i * group, (i + 1) * group))

            else:

                @pl.when(active)
                def _(i=i):
                    stages[i](t)

        return carry

    lax.fori_loop(0, batches + 1, batch_step, 0)

    def finish(m, carry):
        for kind in range(2):
            for j in range(group):

                @pl.when(jnp.logical_and(sends(kind, m, j), me != 2 * kind * group + j))
                def _():
                    input_copy(kind, m, j).wait_send()

        @pl.when(jnp.logical_and(section > 0, m > 0))
        def _():
            for g in range(1, group):
                side_copy(m, g).wait_send()
                side_on(m, g).wait_send()

        def drain(c, carry):
            for g in range(1, group):

                @pl.when(jnp.logical_and(c >= SENT, part_needed(m, c, g)))
                def _():
                    part_copy(m, c, g).wait_send()

            @pl.when(jnp.logical_and(section < LAYERS - 1, keeps(m, c)))
            def _():
                next_copy(m, c).wait_send()

            @pl.when(jnp.logical_and(halved(m), lax.rem(c, group) == member))
            def _():
                for g in range(1, group):
                    relay(m, c, g).wait_send()

            @pl.when(jnp.logical_and(is_cross, lax.rem(c, group) == member))
            def _():
                @pl.when(c // group != 2)
                def _():
                    for g in range(1, group):
                        cross_relay(m, c, g).wait_send()

            @pl.when(jnp.logical_and(is_last, jnp.logical_and(keeps(m, c), me != c)))
            def _():
                out_copy(m, c).wait_send()

            return carry

        lax.fori_loop(0, segs, drain, 0)
        pltpu.make_async_copy(out.at[m], out.at[m], o_recv.at[m]).wait()
        return carry

    lax.fori_loop(0, batches, finish, 0)


def solution(mesh):
    segs = mesh.shape["segment"]

    def on_device(src, tgt, src_len, tgt_len, w_in, w_out, gains, final_gain):
        batches, seq, cw = src.shape
        group = segs // LAYERS
        w_in, w_out = w_in[0], w_out[0]
        width, qkv_cols = w_in.shape
        hc = w_out.shape[0]
        vmem = pl.BlockSpec(memory_space=pltpu.VMEM)
        smem = pl.BlockSpec(memory_space=pltpu.SMEM)
        anym = pl.BlockSpec(memory_space=pl.ANY)
        bf16 = jnp.bfloat16
        block = (segs, seq, cw)
        dma = pltpu.SemaphoreType.DMA
        return pl.pallas_call(
            functools.partial(kernel, segs),
            out_shape=jax.ShapeDtypeStruct(src.shape, src.dtype),
            in_specs=[smem, smem, vmem, vmem, anym, anym, vmem, vmem],
            out_specs=vmem,
            scratch_shapes=[
                pltpu.VMEM((width, qkv_cols), bf16),
                pltpu.VMEM((hc, width), bf16),
                pltpu.VMEM((2, batches) + block, bf16),
                pltpu.VMEM((2, seq, width), bf16),
                pltpu.VMEM((seq, qkv_cols), bf16),
                pltpu.VMEM((seq, hc), bf16),
                pltpu.VMEM(block, jnp.float32),
                pltpu.VMEM((batches,) + block, bf16),
                pltpu.VMEM((batches, group - 1) + block, bf16),
                pltpu.VMEM((batches,) + block, bf16),
                dma((2,)),
                dma((2, batches, segs)),
                dma((2, batches, group)),
                dma((batches, group - 1, segs)),
                dma((batches, group - 1, segs)),
                dma((batches, segs)),
                dma((batches,)),
                pltpu.SemaphoreType.REGULAR((batches - 1,)),
                pltpu.VMEM((batches - 1, group - 1, seq, cw), bf16),
                dma((batches - 1, group - 1)),
                dma((batches - 1, group - 1)),
                dma((batches - 1, group - 1)),
                dma((batches, group - 1, segs)),
                dma((batches, group - 1, segs)),
                pltpu.SemaphoreType.REGULAR,
            ],
            compiler_params=pltpu.CompilerParams(
                collective_id=0,
                has_side_effects=True,
                vmem_limit_bytes=56 * 1024 * 1024,
            ),
        )(src_len, tgt_len, src, tgt, w_in, w_out, gains, final_gain[None])

    return jax.shard_map(
        on_device,
        mesh=mesh,
        in_specs=(
            P("dp", None, "segment"),
            P("dp", None, "segment"),
            P("dp"),
            P("dp"),
            P("segment", None, None),
            P("segment", None, None),
            P(),
            P(),
        ),
        out_specs=P("dp", None, "segment"),
        check_vma=False,
    )
```

```python
import functools

import jax
import jax.numpy as jnp
from jax import lax
from jax.experimental import pallas as pl
from jax.experimental.pallas import tpu as pltpu
from jax.sharding import PartitionSpec as P

HEAD = 64
LAYERS = 4
MESH = pl.DeviceIdType.MESH
TURN = 0
epsilon = 1e-06
score_scale = 0.125


def kernel(
    segs,
    src_len,
    tgt_len,
    src,
    tgt,
    w_in,
    w_out,
    gains,
    final_gain,
    out,
    win,
    wout,
    act,
    nrm,
    qkv,
    mix,
    own,
    ps,
    pr,
    fw,
    side,
    w_sem,
    first_own,
    first_rest,
    later,
    tgt_own,
    tgt_rest,
    in_send,
    p_send,
    p_recv,
    f_send,
    o_recv,
    side_send,
    side_recv,
    on_send,
    r_send,
    t_send,
    go,
    turn,
):
    group = segs // LAYERS
    batches, seq, cw = src.shape
    width = segs * cw
    hc = wout.shape[0]
    me = lax.axis_index("segment")
    section = me // group
    member = me % group
    is_cross = section == 2
    is_last = section == LAYERS - 1
    q_src = jnp.where(is_cross, 1, 0)

    win_copy = pltpu.make_async_copy(w_in, win, w_sem.at[0])
    wout_copy = pltpu.make_async_copy(w_out, wout, w_sem.at[1])
    win_copy.start()
    wout_copy.start()

    barrier = pltpu.get_barrier_semaphore()
    for step in range(1, segs):
        pl.semaphore_signal(
            barrier,
            inc=1,
            device_id={"segment": lax.rem(me + step, segs)},
            device_id_type=MESH,
        )
    lane_at = lax.axis_index("dp")
    leads = lane_at % 2 == 1
    mate = lane_at + 1 - 2 * (lane_at % 2)
    pl.semaphore_signal(
        barrier, inc=1, device_id={"dp": mate}, device_id_type=MESH
    )
    pl.semaphore_wait(barrier, segs)

    def remote(source, dest, send, recv, target):
        return pltpu.make_async_remote_copy(
            src_ref=source,
            dst_ref=dest,
            send_sem=send,
            recv_sem=recv,
            device_id={"segment": target},
            device_id_type=MESH,
        )

    def enc_sem(m, owned, c):
        if isinstance(m, int) and m > 0:
            return later.at[m]
        return first_own.at[c // group] if owned else first_rest.at[0]

    def input_copy(kind, m, j):
        ref = src if kind == 0 else tgt
        target = 2 * kind * group + j
        if kind == 0:
            recv = enc_sem(m, True, me)
        else:
            recv = tgt_own.at[m, section]
        return remote(ref.at[m], act.at[kind, m, me], in_send.at[kind], recv, target)

    def share_copy(m, j):
        return remote(
            tgt.at[m],
            act.at[1, m, me],
            in_send.at[1],
            tgt_rest.at[m],
            2 * group + j,
        )

    def sends(kind, m, j):
        if kind == 1:
            return jnp.logical_or(j == member, is_cross)
        return jnp.logical_or(j == member, jnp.logical_and(section == 0, m > 0))

    def send_inputs(kind, m):
        ref = src if kind == 0 else tgt
        for j in range(group):
            target = 2 * kind * group + j
            wanted = jnp.logical_and(sends(kind, m, j), me != target)
            if kind == 1:

                @pl.when(jnp.logical_and(wanted, is_cross))
                def _():
                    share_copy(m, j).start()

                wanted = jnp.logical_and(wanted, jnp.logical_not(is_cross))

            @pl.when(wanted)
            def _():
                input_copy(kind, m, j).start()

            @pl.when(me == target)
            def _():
                own_sem = enc_sem(m, True, j) if kind == 0 else tgt_own.at[m, 2]
                pltpu.make_async_copy(
                    ref.at[m], act.at[kind, m, me], own_sem
                ).start()

    def beside(g):
        return section * group + lax.rem(member + g, group)

    def side_copy(m, g):
        return remote(
            src.at[m],
            side.at[m - 1, g - 1],
            side_send.at[g - 1],
            side_recv.at[m - 1, g - 1],
            beside(g),
        )

    def side_on(m, g):
        source = beside(group - g)
        return remote(
            side.at[m - 1, g - 1],
            act.at[0, m, source],
            on_send.at[g - 1],
            later.at[m],
            member,
        )

    def relay(c, g):
        return remote(
            act.at[0, 0, c],
            act.at[0, 0, c],
            r_send.at[g - 1],
            first_rest.at[0],
            beside(g),
        )

    def wait_bytes(ref, sem):
        pltpu.make_async_copy(ref, ref, sem).wait()

    send_inputs(0, 0)

    @pl.when(section > 0)
    def _():
        for m in range(1, batches):
            for g in range(1, group):
                side_copy(m, g).start()

    @pl.when(section <= 2)
    def _():
        for m in range(batches):
            send_inputs(1, m)

    def pass_on(order):
        for c in order:

            @pl.when(c % group == member)
            def _(c=c):
                wait_bytes(act.at[0, 0, c], first_own.at[c // group])
                for g in range(1, group):
                    relay(c, g).start()

    def release(k, first):
        for c in range(first * group, segs):

            @pl.when(me != c)
            def _(c=c):
                pl.semaphore_signal(
                    go.at[k - 1],
                    inc=1,
                    device_id={"segment": c},
                    device_id_type=MESH,
                )

    @pl.when(section == 0)
    def _():
        pass_on(tuple(range(group)) + tuple(range(segs - 1, 2 * group - 1, -1)))
        release(1, 0)
        pass_on(range(group, 2 * group))

    def cross_relay(m, c, g):
        return remote(
            act.at[1, m, c],
            act.at[1, m, c],
            t_send.at[g - 1],
            tgt_rest.at[m],
            beside(g),
        )

    def spread_targets(planes):
        for m in range(batches):
            for p in planes:
                for c in range(p * group, (p + 1) * group):

                    @pl.when(jnp.logical_and(is_cross, c % group == member))
                    def _(m=m, c=c, p=p):
                        wait_bytes(act.at[1, m, c], tgt_own.at[m, p])
                        if p != 2:
                            for g in range(1, group):
                                cross_relay(m, c, g).start()

    pl.semaphore_wait(go.at[0], jnp.where(section == 0, group - 1, group))
    for m in range(1, batches):
        if m > 1:
            first = 1 if m == 2 else 2

            @pl.when(section >= first)
            def _(m=m):
                pl.semaphore_wait(go.at[m - 1], group)

        send_inputs(0, m)

        @pl.when(section > 0)
        def _(m=m):
            for g in range(1, group):
                side_copy(m, g).wait_recv()
                side_on(m, g).start()

        if m == 1:

            @pl.when(section > 2)
            def _():
                for k in range(batches):
                    send_inputs(1, k)

            spread_targets((2, 1, 0))

        if m == min(2, batches - 1):
            spread_targets((3,))

    def normalize(kind, m, gain_row):
        total = jnp.zeros((seq, cw), jnp.float32)
        for c in range(segs):
            v = act[kind, m, c].astype(jnp.float32)
            total = total + v * v
        mean = jnp.sum(total, axis=-1, keepdims=True) * (1.0 / width)
        scale = lax.rsqrt(mean + epsilon)
        for c in range(segs):
            v = act[kind, m, c].astype(jnp.float32)
            g = gain_row(c)
            nrm[kind, :, c * cw : (c + 1) * cw] = (v * scale * g).astype(jnp.bfloat16)

    def key_gain(c):
        cols = slice(c * cw, (c + 1) * cw)
        picked = jnp.where(is_cross, final_gain[:, cols], gains[0:1, cols])
        for p in (1, 3):
            picked = jnp.where(section == p, gains[p : p + 1, cols], picked)
        return picked

    def query_gain(c):
        return gains[2:3, c * cw : (c + 1) * cw]

    def part_copy(m, c, g):
        target = section * group + lax.rem(member + g, group)
        return remote(
            ps.at[m, c],
            pr.at[m, g - 1, c],
            p_send.at[m, g - 1, jnp.where(c < group, 0, 1)],
            p_recv.at[m, g - 1, c],
            target,
        )

    def whole_from(p, m):
        inner = m > 0
        return jnp.logical_and(p < LAYERS - 1, inner)

    def whole(m):
        return whole_from(section, m)

    def part_needed(m, c, g):
        goal = lax.rem(member + g, group)
        return jnp.logical_or(whole(m), lax.rem(c, group) == goal)

    def keeps(m, c):
        return jnp.logical_or(whole(m), lax.rem(c, group) == member)

    def next_copy(m, c, recv):
        return remote(fw.at[m, c], act.at[0, m, c], f_send.at[m], recv, me + group)

    def out_copy(m, c):
        return remote(fw.at[m, c], out.at[m], f_send.at[m], o_recv.at[0], c)

    tile = min(512, hc)
    kv_tiles = 2 * hc // tile
    q_tiles = hc // tile

    def prepare(m):
        @pl.when(is_cross)
        def _():
            wait_bytes(act.at[1, m, pl.ds(0, segs - LAYERS)], tgt_rest.at[m])
            normalize(1, m, query_gain)

        @pl.when(jnp.logical_and(section > 0, m == 0))
        def _():
            pass_on(range(segs))

        @pl.when(m == 0)
        def _():
            wait_bytes(act.at[0, 0, pl.ds(0, segs - LAYERS)], first_rest.at[0])

        @pl.when(m > 0)
        def _():
            wait_bytes(act.at[0, m], later.at[m])

        normalize(0, m, key_gain)
        @pl.when(m == 0)
        def _():
            win_copy.wait()

    def project(t, carry):
        kind = jnp.where(t < q_tiles, q_src, 0)
        cols = pl.ds(pl.multiple_of(t * tile, tile), tile)
        qkv[:, cols] = jnp.dot(
            nrm[kind], win[:, cols], preferred_element_type=jnp.float32
        ).astype(jnp.bfloat16)
        return carry

    def attend(m, pairs):
        length = jnp.where(is_last, tgt_len[m], src_len[m])
        keys = lax.broadcasted_iota(jnp.int32, (2 * seq, seq), 1)
        rows = lax.broadcasted_iota(jnp.int32, (2 * seq, seq), 0)
        rows = jnp.where(rows >= seq, rows - seq, rows)
        bound = jnp.where(is_last, rows, seq)
        allowed = (keys < length) & (keys <= bound)
        lane = lax.broadcasted_iota(jnp.int32, (seq, 2 * HEAD), 1)
        low = lane < HEAD
        for h in pairs:
            at = h * 2 * HEAD
            q2 = qkv[:, at : at + 2 * HEAD]
            k2 = qkv[:, hc + at : hc + at + 2 * HEAD]
            v2 = qkv[:, 2 * hc + at : 2 * hc + at + 2 * HEAD]
            zero = jnp.zeros_like(q2)
            both = jnp.concatenate(
                [jnp.where(low, q2, zero), jnp.where(low, zero, q2)], axis=0
            )
            scores = (
                lax.dot_general(
                    both,
                    k2,
                    (((1,), (1,)), ((), ())),
                    preferred_element_type=jnp.float32,
                )
                * score_scale
            )
            scores = jnp.where(allowed, scores, -1000000000.0)
            top = jnp.max(scores, axis=-1, keepdims=True)
            e = jnp.exp(scores - top)
            weights = (e / jnp.sum(e, axis=-1, keepdims=True)).astype(jnp.bfloat16)
            o = jnp.dot(weights, v2, preferred_element_type=jnp.float32)
            mix[:, at : at + 2 * HEAD] = jnp.where(low, o[:seq], o[seq:]).astype(
                jnp.bfloat16
            )

    def send_parts(m):
        @pl.when(m == 0)
        def _():
            wout_copy.wait()

        def emit(c, carry):
            cols = pl.ds(pl.multiple_of(c * cw, cw), cw)
            part = jnp.dot(mix[...], wout[:, cols], preferred_element_type=jnp.float32)
            own[c] = part
            ps[m, c] = part.astype(jnp.bfloat16)

            @pl.when(jnp.logical_and(c == 0, jnp.logical_or(m > 0, jnp.logical_not(leads))))
            def _():
                pl.semaphore_wait(turn, 1)

            for g in range(1, group):

                @pl.when(part_needed(m, c, g))
                def _():
                    part_copy(m, c, g).start()

            return carry

        lax.fori_loop(0, segs, emit, 0, unroll=True)

    def part_sends(m, at, count, count_half):
        for g in range(1, group):
            sem = p_send.at[m, g - 1, at]

            @pl.when(whole(m))
            def _():
                wait_bytes(ps.at[m, pl.ds(0, count)], sem)

            @pl.when(jnp.logical_not(whole(m)))
            def _():
                wait_bytes(ps.at[m, pl.ds(0, count_half)], sem)

    def hand_over(m):
        part_sends(m, 0, group, 1)

        @pl.when(jnp.logical_or(m < batches - 1, leads))
        def _():
            pl.semaphore_signal(
                turn, inc=1, device_id={"dp": mate}, device_id_type=MESH
            )

    def combine(m, c):
        @pl.when(keeps(m, c))
        def _():
            total = own[c] + act[q_src, m, c].astype(jnp.float32)
            for g in range(1, group):
                part_copy(m, c, g).wait_recv()
                total = total + pr[m, g - 1, c].astype(jnp.float32)
            fw[m, c] = total.astype(jnp.bfloat16)

            onward = section < LAYERS - 1

            @pl.when(jnp.logical_and(onward, m == 0))
            def _():
                next_copy(m, c, first_own.at[c // group]).start()

            @pl.when(jnp.logical_and(onward, m > 0))
            def _():
                next_copy(m, c, later.at[m]).start()

            @pl.when(jnp.logical_and(is_last, me != c))
            def _():
                out_copy(m, c).start()

            @pl.when(jnp.logical_and(is_last, me == c))
            def _():
                pltpu.make_async_copy(fw.at[m, c], out.at[m], o_recv.at[0]).start()

    tiles = q_tiles + kv_tiles
    head_pairs = hc // (2 * HEAD)

    def run(step, m, t):
        kind, i, n = step
        if kind == "turn":
            pl.when(t > 0)(lambda: hand_over(m))
        elif kind == "combine":
            pl.when(t > 0)(lambda: combine(m, i))
        elif kind == "prepare":
            pl.when(t < batches)(lambda: prepare(t))
        elif kind == "project":

            @pl.when(t < batches)
            def _():
                lo, hi = i * tiles // n, (i + 1) * tiles // n
                lax.fori_loop(lo, hi, project, 0, unroll=True)

        else:

            @pl.when(t < batches)
            def _():
                attend(t, range(i * head_pairs // n, (i + 1) * head_pairs // n))

    combines = [("combine", c, segs) for c in range(segs)]
    turn_at = min(TURN, segs - 1)
    steps = combines[:turn_at] + [("turn", 0, 1)] + combines[turn_at:]
    steps += [("prepare", 0, 1)]
    steps += [("project", 0, 2), ("project", 1, 2), ("attend", 0, 1)]

    def batch_step(t, carry):
        m = t - 1

        @pl.when(t > 0)
        def _():
            send_parts(m)

        for k in range(2, batches):

            @pl.when(jnp.logical_and(section == 0, t == k - 1))
            def _(k=k):
                release(k, 1 if k == 2 else 2)

        for step in steps:
            run(step, m, t)

        return carry

    lax.fori_loop(0, batches + 1, batch_step, 0)

    def forward_sends(m):
        for ahead, count in ((whole(m), segs), (jnp.logical_not(whole(m)), LAYERS)):

            @pl.when(jnp.logical_and(section < LAYERS - 1, ahead))
            def _(count=count):
                wait_bytes(fw.at[m, pl.ds(0, count)], f_send.at[m])

        @pl.when(is_last)
        def _():
            wait_bytes(fw.at[m, pl.ds(0, LAYERS - 1)], f_send.at[m])

    some = pl.ds(0, batches - 1)
    for m in range(batches):
        part_sends(m, 1, segs - group, LAYERS - 1)
        forward_sends(m)

    @pl.when(section > 0)
    def _():
        wait_bytes(src, in_send.at[0])
        for g in range(1, group):
            wait_bytes(src.at[some], side_send.at[g - 1])
            wait_bytes(src.at[some], on_send.at[g - 1])

    @pl.when(section == 0)
    def _():
        for g in range(1, group):
            wait_bytes(src.at[some], in_send.at[0])

    @pl.when(jnp.logical_not(is_cross))
    def _():
        wait_bytes(tgt, in_send.at[1])

    for g in range(1, group):
        wait_bytes(act.at[0, 0, pl.ds(0, LAYERS)], r_send.at[g - 1])

        @pl.when(is_cross)
        def _(g=g):
            wait_bytes(tgt, in_send.at[1])
            wait_bytes(act.at[1, :, pl.ds(0, LAYERS - 1)], t_send.at[g - 1])

    wait_bytes(out, o_recv.at[0])


def solution(mesh):
    segs = mesh.shape["segment"]

    def on_device(src, tgt, src_len, tgt_len, w_in, w_out, gains, final_gain):
        batches, seq, cw = src.shape
        group = segs // LAYERS
        w_in, w_out = w_in[0], w_out[0]
        width, qkv_cols = w_in.shape
        hc = w_out.shape[0]
        vmem = pl.BlockSpec(memory_space=pltpu.VMEM)
        smem = pl.BlockSpec(memory_space=pltpu.SMEM)
        anym = pl.BlockSpec(memory_space=pl.ANY)
        bf16 = jnp.bfloat16
        block = (segs, seq, cw)
        dma = pltpu.SemaphoreType.DMA
        return pl.pallas_call(
            functools.partial(kernel, segs),
            out_shape=pltpu.VMEM(src.shape, src.dtype),
            in_specs=[smem, smem, vmem, vmem, anym, anym, vmem, vmem],
            out_specs=vmem,
            scratch_shapes=[
                pltpu.VMEM((width, qkv_cols), bf16),
                pltpu.VMEM((hc, width), bf16),
                pltpu.VMEM((2, batches) + block, bf16),
                pltpu.VMEM((2, seq, width), bf16),
                pltpu.VMEM((seq, qkv_cols), bf16),
                pltpu.VMEM((seq, hc), bf16),
                pltpu.VMEM(block, jnp.float32),
                pltpu.VMEM((batches,) + block, bf16),
                pltpu.VMEM((batches, group - 1) + block, bf16),
                pltpu.VMEM((batches,) + block, bf16),
                pltpu.VMEM((batches - 1, group - 1, seq, cw), bf16),
                dma((2,)),
                dma((LAYERS,)),
                dma((1,)),
                dma((batches,)),
                dma((batches, LAYERS)),
                dma((batches,)),
                dma((2,)),
                dma((batches, group - 1, 2)),
                dma((batches, group - 1, segs)),
                dma((batches,)),
                dma((1,)),
                dma((group - 1,)),
                dma((batches - 1, group - 1)),
                dma((group - 1,)),
                dma((group - 1,)),
                dma((group - 1,)),
                pltpu.SemaphoreType.REGULAR((batches - 1,)),
                pltpu.SemaphoreType.REGULAR,
            ],
            compiler_params=pltpu.CompilerParams(
                collective_id=0,
                has_side_effects=True,
                vmem_limit_bytes=56 * 1024 * 1024,
            ),
        )(src_len, tgt_len, src, tgt, w_in, w_out, gains, final_gain[None])

    return jax.shard_map(
        on_device,
        mesh=mesh,
        in_specs=(
            P("dp", None, "segment"),
            P("dp", None, "segment"),
            P("dp"),
            P("dp"),
            P("segment", None, None),
            P("segment", None, None),
            P(),
            P(),
        ),
        out_specs=P("dp", None, "segment"),
        check_vma=False,
    )
```

```python
import functools

import jax
import jax.numpy as jnp
from jax import lax
from jax.experimental import pallas as pl
from jax.experimental.pallas import tpu as pltpu
from jax.sharding import PartitionSpec as P

HEAD = 64
LAYERS = 4
MESH = pl.DeviceIdType.MESH
TURN = 0
epsilon = 1e-06
score_scale = 0.125


def kernel(
    segs,
    src_len,
    tgt_len,
    src,
    tgt,
    w_in,
    w_out,
    gains,
    final_gain,
    out,
    win,
    wout,
    act,
    nrm,
    qkv,
    mix,
    own,
    ps,
    pr,
    fw,
    side,
    acc,
    w_sem,
    first_own,
    first_rest,
    later,
    tgt_own,
    tgt_rest,
    in_send,
    p_send,
    p_recv,
    f_send,
    o_recv,
    side_send,
    side_recv,
    on_send,
    r_send,
    t_send,
    go,
    turn,
):
    group = segs // LAYERS
    batches, seq, cw = src.shape
    width = segs * cw
    hc = wout.shape[0]
    me = lax.axis_index("segment")
    section = me // group
    member = me % group
    is_cross = section == 2
    is_last = section == LAYERS - 1
    q_src = jnp.where(is_cross, 1, 0)

    win_copy = pltpu.make_async_copy(w_in, win, w_sem.at[0])
    wout_copy = pltpu.make_async_copy(w_out, wout, w_sem.at[1])
    win_copy.start()
    wout_copy.start()

    barrier = pltpu.get_barrier_semaphore()
    for step in range(1, segs):
        pl.semaphore_signal(
            barrier,
            inc=1,
            device_id={"segment": lax.rem(me + step, segs)},
            device_id_type=MESH,
        )
    lane_at = lax.axis_index("dp")
    leads = lane_at % 2 == 1
    mate = lane_at + 1 - 2 * (lane_at % 2)
    pl.semaphore_signal(
        barrier, inc=1, device_id={"dp": mate}, device_id_type=MESH
    )
    pl.semaphore_wait(barrier, segs)

    def remote(source, dest, send, recv, target):
        return pltpu.make_async_remote_copy(
            src_ref=source,
            dst_ref=dest,
            send_sem=send,
            recv_sem=recv,
            device_id={"segment": target},
            device_id_type=MESH,
        )

    def enc_sem(m, c):
        if isinstance(m, int) and m > 0:
            return later.at[m]
        return first_own.at[c // group]

    def input_copy(kind, m, j):
        ref = src if kind == 0 else tgt
        target = 2 * kind * group + j
        if kind == 0:
            recv = enc_sem(m, me)
        else:
            recv = tgt_own.at[m, section]
        return remote(ref.at[m], act.at[kind, m, me], in_send.at[kind], recv, target)

    def share_copy(m, j):
        return remote(
            tgt.at[m],
            act.at[1, m, me],
            in_send.at[1],
            tgt_rest.at[m],
            2 * group + j,
        )

    def sends(kind, m, j):
        if kind == 1:
            return jnp.logical_or(j == member, is_cross)
        return jnp.logical_or(j == member, jnp.logical_and(section == 0, m > 0))

    def send_inputs(kind, m):
        ref = src if kind == 0 else tgt
        for j in range(group):
            target = 2 * kind * group + j
            wanted = jnp.logical_and(sends(kind, m, j), me != target)
            if kind == 1:

                @pl.when(jnp.logical_and(wanted, is_cross))
                def _():
                    share_copy(m, j).start()

                wanted = jnp.logical_and(wanted, jnp.logical_not(is_cross))

            @pl.when(wanted)
            def _():
                input_copy(kind, m, j).start()

            @pl.when(me == target)
            def _():
                own_sem = enc_sem(m, j) if kind == 0 else tgt_own.at[m, 2]
                pltpu.make_async_copy(
                    ref.at[m], act.at[kind, m, me], own_sem
                ).start()

    def beside(g):
        return section * group + lax.rem(member + g, group)

    def side_copy(m, g):
        return remote(
            src.at[m],
            side.at[m - 1, g - 1],
            side_send.at[g - 1],
            side_recv.at[m - 1, g - 1],
            beside(g),
        )

    def side_on(m, g):
        source = beside(group - g)
        return remote(
            side.at[m - 1, g - 1],
            act.at[0, m, source],
            on_send.at[g - 1],
            later.at[m],
            member,
        )

    def relay(c, g):
        return remote(
            act.at[0, 0, c],
            act.at[0, 0, c],
            r_send.at[g - 1],
            first_rest.at[c],
            beside(g),
        )

    def wait_bytes(ref, sem):
        pltpu.make_async_copy(ref, ref, sem).wait()

    send_inputs(0, 0)

    @pl.when(section > 0)
    def _():
        for m in range(1, batches):
            for g in range(1, group):
                side_copy(m, g).start()

    @pl.when(section <= 2)
    def _():
        for m in range(batches):
            send_inputs(1, m)

    def pass_on(order):
        for c in order:

            @pl.when(c % group == member)
            def _(c=c):
                wait_bytes(act.at[0, 0, c], first_own.at[c // group])
                for g in range(1, group):
                    relay(c, g).start()

    def release(k, first):
        for c in range(first * group, segs):

            @pl.when(me != c)
            def _(c=c):
                pl.semaphore_signal(
                    go.at[k - 1],
                    inc=1,
                    device_id={"segment": c},
                    device_id_type=MESH,
                )

    @pl.when(section == 0)
    def _():
        pass_on(range(group))
        send_inputs(0, 1)
        pass_on(range(segs - 1, 2 * group - 1, -1))
        release(1, 0)
        pass_on(range(group, 2 * group))

    def cross_relay(m, c, g):
        return remote(
            act.at[1, m, c],
            act.at[1, m, c],
            t_send.at[g - 1],
            tgt_rest.at[m],
            beside(g),
        )

    def spread_targets(planes):
        for m in range(batches):
            for p in planes:
                for c in range(p * group, (p + 1) * group):

                    @pl.when(jnp.logical_and(is_cross, c % group == member))
                    def _(m=m, c=c, p=p):
                        wait_bytes(act.at[1, m, c], tgt_own.at[m, p])
                        if p != 2:
                            for g in range(1, group):
                                cross_relay(m, c, g).start()

    pl.semaphore_wait(go.at[0], jnp.where(section == 0, group - 1, group))
    for m in range(1, batches):
        if m > 1:
            first = 1 if m == 2 else 2

            @pl.when(section >= first)
            def _(m=m):
                pl.semaphore_wait(go.at[m - 1], group)

        @pl.when(section > 0)
        def _(m=m):
            send_inputs(0, m)

        @pl.when(section > 0)
        def _(m=m):
            for g in range(1, group):
                side_copy(m, g).wait_recv()
                side_on(m, g).start()

        if m == 1:

            @pl.when(section > 2)
            def _():
                for k in range(batches):
                    send_inputs(1, k)

            spread_targets((2, 1, 0))

        if m == min(2, batches - 1):
            spread_targets((3,))

    def normalize(kind, m, gain_row):
        total = jnp.zeros((seq, cw), jnp.float32)
        for c in range(segs):
            v = act[kind, m, c].astype(jnp.float32)
            total = total + v * v
        mean = jnp.sum(total, axis=-1, keepdims=True) * (1.0 / width)
        scale = lax.rsqrt(mean + epsilon)
        for c in range(segs):
            v = act[kind, m, c].astype(jnp.float32)
            g = gain_row(c)
            nrm[kind, :, c * cw : (c + 1) * cw] = (v * scale * g).astype(jnp.bfloat16)

    def key_gain(c):
        cols = pl.ds(pl.multiple_of(c * cw, cw), cw)
        picked = jnp.where(is_cross, final_gain[:, cols], gains[0:1, cols])
        for p in (1, 3):
            picked = jnp.where(section == p, gains[p : p + 1, cols], picked)
        return picked

    def query_gain(c):
        return gains[2:3, c * cw : (c + 1) * cw]

    def part_copy(m, c, g):
        target = section * group + lax.rem(member + g, group)
        return remote(
            ps.at[m, c],
            pr.at[m, g - 1, c],
            p_send.at[m, g - 1, jnp.where(c < group, 0, 1)],
            p_recv.at[m, g - 1, c],
            target,
        )

    def whole_from(p, m):
        inner = m > 0
        return jnp.logical_and(p < LAYERS - 1, inner)

    def whole(m):
        return whole_from(section, m)

    def part_needed(m, c, g):
        goal = lax.rem(member + g, group)
        return jnp.logical_or(whole(m), lax.rem(c, group) == goal)

    def keeps(m, c):
        return jnp.logical_or(whole(m), lax.rem(c, group) == member)

    def next_copy(m, c, recv):
        return remote(fw.at[m, c], act.at[0, m, c], f_send.at[m], recv, me + group)

    def out_copy(m, c):
        return remote(fw.at[m, c], out.at[m], f_send.at[m], o_recv.at[0], c)

    def prepare(m):
        @pl.when(is_cross)
        def _():
            wait_bytes(act.at[1, m, pl.ds(0, segs - LAYERS)], tgt_rest.at[m])
            normalize(1, m, query_gain)

        @pl.when(m > 0)
        def _():
            wait_bytes(act.at[0, m], later.at[m])
            normalize(0, m, key_gain)

    def project(at, width_at):
        kind = q_src if at < hc else 0
        cols = slice(at, at + width_at)
        qkv[:, cols] = jnp.dot(
            nrm[kind], win[:, cols], preferred_element_type=jnp.float32
        ).astype(jnp.bfloat16)

    def attend(m, pairs):
        length = jnp.where(is_last, tgt_len[m], src_len[m])
        keys = lax.broadcasted_iota(jnp.int32, (2 * seq, seq), 1)
        rows = lax.broadcasted_iota(jnp.int32, (2 * seq, seq), 0)
        rows = jnp.where(rows >= seq, rows - seq, rows)
        bound = jnp.where(is_last, rows, seq)
        allowed = (keys < length) & (keys <= bound)
        lane = lax.broadcasted_iota(jnp.int32, (seq, 2 * HEAD), 1)
        low = lane < HEAD
        for h in pairs:
            at = h * 2 * HEAD
            q2 = qkv[:, at : at + 2 * HEAD]
            k2 = qkv[:, hc + at : hc + at + 2 * HEAD]
            v2 = qkv[:, 2 * hc + at : 2 * hc + at + 2 * HEAD]
            zero = jnp.zeros_like(q2)
            both = jnp.concatenate(
                [jnp.where(low, q2, zero), jnp.where(low, zero, q2)], axis=0
            )
            scores = (
                lax.dot_general(
                    both,
                    k2,
                    (((1,), (1,)), ((), ())),
                    preferred_element_type=jnp.float32,
                )
                * score_scale
            )
            scores = jnp.where(allowed, scores, -1000000000.0)
            top = jnp.max(scores, axis=-1, keepdims=True)
            e = jnp.exp(scores - top)
            weights = (e * (1.0 / jnp.sum(e, axis=-1, keepdims=True))).astype(jnp.bfloat16)
            o = jnp.dot(weights, v2, preferred_element_type=jnp.float32)
            mix[:, at : at + 2 * HEAD] = jnp.where(low, o[:seq], o[seq:]).astype(
                jnp.bfloat16
            )

    def send_parts(m):
        @pl.when(m == 0)
        def _():
            wout_copy.wait()

        def emit(c, carry):
            cols = pl.ds(pl.multiple_of(c * cw, cw), cw)
            part = jnp.dot(mix[...], wout[:, cols], preferred_element_type=jnp.float32)
            own[c] = part
            ps[m, c] = part.astype(jnp.bfloat16)

            @pl.when(jnp.logical_and(c == 0, jnp.logical_or(m > 0, jnp.logical_not(leads))))
            def _():
                pl.semaphore_wait(turn, 1)

            for g in range(1, group):

                @pl.when(part_needed(m, c, g))
                def _():
                    part_copy(m, c, g).start()

            return carry

        lax.fori_loop(0, segs, emit, 0, unroll=True)

    def part_sends(m, at, count, count_half):
        for g in range(1, group):
            sem = p_send.at[m, g - 1, at]

            @pl.when(whole(m))
            def _():
                wait_bytes(ps.at[m, pl.ds(0, count)], sem)

            @pl.when(jnp.logical_not(whole(m)))
            def _():
                wait_bytes(ps.at[m, pl.ds(0, count_half)], sem)

    def hand_over(m):
        part_sends(m, 0, group, 1)

        @pl.when(jnp.logical_or(m < batches - 1, leads))
        def _():
            pl.semaphore_signal(
                turn, inc=1, device_id={"dp": mate}, device_id_type=MESH
            )

    def combine(m, c):
        @pl.when(keeps(m, c))
        def _():
            total = own[c] + act[q_src, m, c].astype(jnp.float32)
            for g in range(1, group):
                part_copy(m, c, g).wait_recv()
                total = total + pr[m, g - 1, c].astype(jnp.float32)
            fw[m, c] = total.astype(jnp.bfloat16)

            onward = section < LAYERS - 1

            @pl.when(jnp.logical_and(onward, m == 0))
            def _():
                next_copy(m, c, first_own.at[c // group]).start()

            @pl.when(jnp.logical_and(onward, m > 0))
            def _():
                next_copy(m, c, later.at[m]).start()

            @pl.when(jnp.logical_and(is_last, me != c))
            def _():
                out_copy(m, c).start()

            @pl.when(jnp.logical_and(is_last, me == c))
            def _():
                pltpu.make_async_copy(fw.at[m, c], out.at[m], o_recv.at[0]).start()

    head_pairs = hc // (2 * HEAD)
    tile = min(512, hc)

    def add_chunk(c, first):
        v = act[0, 0, c].astype(jnp.float32)
        square = v * v
        own[0] = square if first else own[0] + square
        scaled = (v * key_gain(c)).astype(jnp.bfloat16)
        rows = pl.ds(pl.multiple_of(c * cw, cw), cw)
        for at in range(0, 3 * hc, tile):
            cols = slice(at, at + tile)
            part = jnp.dot(
                scaled, win[rows, cols], preferred_element_type=jnp.float32
            )
            acc[:, cols] = part if first else acc[:, cols] + part

    def start_up():
        @pl.when(section == 0)
        def _():
            for k in range(2, batches):
                send_inputs(0, k)

        win_copy.wait()

        @pl.when(is_cross)
        def _():
            for at in range(0, hc, tile):
                project(at, tile)

        for i in range(LAYERS):
            c = i * group + member

            @pl.when(section > 0)
            def _(i=i, c=c):
                wait_bytes(act.at[0, 0, c], first_own.at[i])
                for g in range(1, group):
                    relay(c, g).start()

            add_chunk(c, i == 0)
        for i in range(LAYERS):
            for g in range(1, group):
                c = i * group + lax.rem(member + g, group)
                wait_bytes(act.at[0, 0, c], first_rest.at[c])
                add_chunk(c, False)
        mean = jnp.sum(own[0], axis=-1, keepdims=True) * (1.0 / width)
        scale = lax.rsqrt(mean + epsilon)

        @pl.when(jnp.logical_not(is_cross))
        def _():
            qkv[:, :hc] = (acc[:, :hc] * scale).astype(jnp.bfloat16)

        qkv[:, hc:] = (acc[:, hc:] * scale).astype(jnp.bfloat16)

    def compute(m):
        @pl.when(m == 0)
        def _():
            start_up()
            attend(m, range(head_pairs))

        @pl.when(m > 0)
        def _():
            for at in range(0, 3 * hc, tile):
                project(at, tile)
            attend(m, range(head_pairs))

    def run(step, m, t):
        kind, i, n = step
        if kind == "turn":
            pl.when(t > 0)(lambda: hand_over(m))
        elif kind == "combine":
            pl.when(t > 0)(lambda: combine(m, i))
        elif kind == "prepare":
            pl.when(t < batches)(lambda: prepare(t))
        else:
            pl.when(t < batches)(lambda: compute(t))

    combines = [("combine", c, segs) for c in range(segs)]
    turn_at = min(TURN, segs - 1)
    steps = combines[:turn_at] + [("turn", 0, 1)] + combines[turn_at:]
    steps += [("prepare", 0, 1), ("compute", 0, 1)]

    def batch_step(t, carry):
        m = t - 1

        @pl.when(t > 0)
        def _():
            send_parts(m)

        for k in range(2, batches):

            @pl.when(jnp.logical_and(section == 0, t == k - 1))
            def _(k=k):
                release(k, 1 if k == 2 else 2)

        for step in steps:
            run(step, m, t)

        return carry

    lax.fori_loop(0, batches + 1, batch_step, 0)

    def forward_sends(m):
        for ahead, count in ((whole(m), segs), (jnp.logical_not(whole(m)), LAYERS)):

            @pl.when(jnp.logical_and(section < LAYERS - 1, ahead))
            def _(count=count):
                wait_bytes(fw.at[m, pl.ds(0, count)], f_send.at[m])

        @pl.when(is_last)
        def _():
            wait_bytes(fw.at[m, pl.ds(0, LAYERS - 1)], f_send.at[m])

    some = pl.ds(0, batches - 1)
    for m in range(batches):
        part_sends(m, 1, segs - group, LAYERS - 1)
        forward_sends(m)

    @pl.when(section > 0)
    def _():
        wait_bytes(src, in_send.at[0])
        for g in range(1, group):
            wait_bytes(src.at[some], side_send.at[g - 1])
            wait_bytes(src.at[some], on_send.at[g - 1])

    @pl.when(section == 0)
    def _():
        for g in range(1, group):
            wait_bytes(src.at[some], in_send.at[0])

    @pl.when(jnp.logical_not(is_cross))
    def _():
        wait_bytes(tgt, in_send.at[1])

    for g in range(1, group):
        wait_bytes(act.at[0, 0, pl.ds(0, LAYERS)], r_send.at[g - 1])

        @pl.when(is_cross)
        def _(g=g):
            wait_bytes(tgt, in_send.at[1])
            wait_bytes(act.at[1, :, pl.ds(0, LAYERS - 1)], t_send.at[g - 1])

    wait_bytes(out, o_recv.at[0])


def solution(mesh):
    segs = mesh.shape["segment"]

    def on_device(src, tgt, src_len, tgt_len, w_in, w_out, gains, final_gain):
        batches, seq, cw = src.shape
        group = segs // LAYERS
        w_in, w_out = w_in[0], w_out[0]
        width, qkv_cols = w_in.shape
        hc = w_out.shape[0]
        vmem = pl.BlockSpec(memory_space=pltpu.VMEM)
        smem = pl.BlockSpec(memory_space=pltpu.SMEM)
        anym = pl.BlockSpec(memory_space=pl.ANY)
        bf16 = jnp.bfloat16
        block = (segs, seq, cw)
        dma = pltpu.SemaphoreType.DMA
        return pl.pallas_call(
            functools.partial(kernel, segs),
            out_shape=pltpu.VMEM(src.shape, src.dtype),
            in_specs=[smem, smem, vmem, vmem, anym, anym, vmem, vmem],
            out_specs=vmem,
            scratch_shapes=[
                pltpu.VMEM((width, qkv_cols), bf16),
                pltpu.VMEM((hc, width), bf16),
                pltpu.VMEM((2, batches) + block, bf16),
                pltpu.VMEM((2, seq, width), bf16),
                pltpu.VMEM((seq, qkv_cols), bf16),
                pltpu.VMEM((seq, hc), bf16),
                pltpu.VMEM(block, jnp.float32),
                pltpu.VMEM((batches,) + block, bf16),
                pltpu.VMEM((batches, group - 1) + block, bf16),
                pltpu.VMEM((batches,) + block, bf16),
                pltpu.VMEM((batches - 1, group - 1, seq, cw), bf16),
                pltpu.VMEM((seq, qkv_cols), jnp.float32),
                dma((2,)),
                dma((LAYERS,)),
                dma((segs,)),
                dma((batches,)),
                dma((batches, LAYERS)),
                dma((batches,)),
                dma((2,)),
                dma((batches, group - 1, 2)),
                dma((batches, group - 1, segs)),
                dma((batches,)),
                dma((1,)),
                dma((group - 1,)),
                dma((batches - 1, group - 1)),
                dma((group - 1,)),
                dma((group - 1,)),
                dma((group - 1,)),
                pltpu.SemaphoreType.REGULAR((batches - 1,)),
                pltpu.SemaphoreType.REGULAR,
            ],
            compiler_params=pltpu.CompilerParams(
                collective_id=0,
                has_side_effects=True,
                vmem_limit_bytes=56 * 1024 * 1024,
            ),
        )(src_len, tgt_len, src, tgt, w_in, w_out, gains, final_gain[None])

    return jax.shard_map(
        on_device,
        mesh=mesh,
        in_specs=(
            P("dp", None, "segment"),
            P("dp", None, "segment"),
            P("dp"),
            P("dp"),
            P("segment", None, None),
            P("segment", None, None),
            P(),
            P(),
        ),
        out_specs=P("dp", None, "segment"),
        check_vma=False,
    )
```

```python
import functools

import jax
import jax.numpy as jnp
from jax import lax
from jax.experimental import pallas as pl
from jax.experimental.pallas import tpu as pltpu
from jax.sharding import PartitionSpec as P

HEAD = 64
LAYERS = 4
MESH = pl.DeviceIdType.MESH
TURN = 0
epsilon = 1e-06
score_scale = 0.125


def kernel(
    segs,
    src_len,
    tgt_len,
    src,
    tgt,
    w_in,
    w_out,
    gains,
    final_gain,
    out,
    win,
    wout,
    act,
    nrm,
    qkv,
    mix,
    own,
    ps,
    pr,
    fw,
    side,
    acc,
    w_sem,
    first_own,
    first_rest,
    later,
    tgt_own,
    tgt_rest,
    in_send,
    p_send,
    p_recv,
    f_send,
    o_recv,
    side_send,
    side_recv,
    on_send,
    r_send,
    t_send,
    go,
    turn,
):
    group = segs // LAYERS
    batches, seq, cw = src.shape
    width = segs * cw
    hc = wout.shape[0]
    me = lax.axis_index("segment")
    section = me // group
    member = me % group
    is_cross = section == 2
    is_last = section == LAYERS - 1
    q_src = jnp.where(is_cross, 1, 0)

    win_copy = pltpu.make_async_copy(w_in, win, w_sem.at[0])
    wout_copy = pltpu.make_async_copy(w_out, wout, w_sem.at[1])
    win_copy.start()
    wout_copy.start()

    barrier = pltpu.get_barrier_semaphore()
    for step in range(1, segs):
        pl.semaphore_signal(
            barrier,
            inc=1,
            device_id={"segment": lax.rem(me + step, segs)},
            device_id_type=MESH,
        )
    lane_at = lax.axis_index("dp")
    leads = lane_at % 2 == 1
    mate = lane_at + 1 - 2 * (lane_at % 2)
    pl.semaphore_signal(
        barrier, inc=1, device_id={"dp": mate}, device_id_type=MESH
    )
    pl.semaphore_wait(barrier, segs)

    def remote(source, dest, send, recv, target):
        return pltpu.make_async_remote_copy(
            src_ref=source,
            dst_ref=dest,
            send_sem=send,
            recv_sem=recv,
            device_id={"segment": target},
            device_id_type=MESH,
        )

    def enc_sem(m, c):
        if isinstance(m, int) and m > 0:
            return later.at[m]
        return first_own.at[c // group]

    def input_copy(kind, m, j):
        ref = src if kind == 0 else tgt
        target = 2 * kind * group + j
        if kind == 0:
            recv = enc_sem(m, me)
        else:
            recv = tgt_own.at[m, section]
        return remote(ref.at[m], act.at[kind, m, me], in_send.at[kind], recv, target)

    def share_copy(m, j):
        return remote(
            tgt.at[m],
            act.at[1, m, me],
            in_send.at[1],
            tgt_rest.at[m],
            2 * group + j,
        )

    def sends(kind, m, j):
        if kind == 1:
            return jnp.logical_or(j == member, is_cross)
        return jnp.logical_or(j == member, jnp.logical_and(section == 0, m > 0))

    def send_inputs(kind, m):
        ref = src if kind == 0 else tgt
        for j in range(group):
            target = 2 * kind * group + j
            wanted = jnp.logical_and(sends(kind, m, j), me != target)
            if kind == 1:

                @pl.when(jnp.logical_and(wanted, is_cross))
                def _():
                    share_copy(m, j).start()

                wanted = jnp.logical_and(wanted, jnp.logical_not(is_cross))

            @pl.when(wanted)
            def _():
                input_copy(kind, m, j).start()

            @pl.when(me == target)
            def _():
                own_sem = enc_sem(m, j) if kind == 0 else tgt_own.at[m, 2]
                pltpu.make_async_copy(
                    ref.at[m], act.at[kind, m, me], own_sem
                ).start()

    def beside(g):
        return section * group + lax.rem(member + g, group)

    def side_copy(m, g):
        return remote(
            src.at[m],
            side.at[m - 1, g - 1],
            side_send.at[g - 1],
            side_recv.at[m - 1, g - 1],
            beside(g),
        )

    def side_on(m, g):
        source = beside(group - g)
        return remote(
            side.at[m - 1, g - 1],
            act.at[0, m, source],
            on_send.at[g - 1],
            later.at[m],
            member,
        )

    def relay(c, g):
        return remote(
            act.at[0, 0, c],
            act.at[0, 0, c],
            r_send.at[g - 1],
            first_rest.at[c],
            beside(g),
        )

    def wait_bytes(ref, sem):
        pltpu.make_async_copy(ref, ref, sem).wait()

    send_inputs(0, 0)

    @pl.when(section > 0)
    def _():
        for m in range(1, batches):
            for g in range(1, group):
                side_copy(m, g).start()

    @pl.when(section <= 2)
    def _():
        for m in range(batches):
            send_inputs(1, m)

    def pass_on(order):
        for c in order:

            @pl.when(c % group == member)
            def _(c=c):
                wait_bytes(act.at[0, 0, c], first_own.at[c // group])
                for g in range(1, group):
                    relay(c, g).start()

    def release(k, first):
        for c in range(first * group, segs):

            @pl.when(me != c)
            def _(c=c):
                pl.semaphore_signal(
                    go.at[k - 1],
                    inc=1,
                    device_id={"segment": c},
                    device_id_type=MESH,
                )

    @pl.when(section == 0)
    def _():
        pass_on(range(group))
        send_inputs(0, 1)
        pass_on(range(segs - 1, 2 * group - 1, -1))
        release(1, 0)
        pass_on(range(group, 2 * group))

    def cross_relay(m, c, g):
        return remote(
            act.at[1, m, c],
            act.at[1, m, c],
            t_send.at[g - 1],
            tgt_rest.at[m],
            beside(g),
        )

    def spread_targets(planes):
        for m in range(batches):
            for p in planes:
                for c in range(p * group, (p + 1) * group):

                    @pl.when(jnp.logical_and(is_cross, c % group == member))
                    def _(m=m, c=c, p=p):
                        wait_bytes(act.at[1, m, c], tgt_own.at[m, p])
                        if p != 2:
                            for g in range(1, group):
                                cross_relay(m, c, g).start()

    pl.semaphore_wait(go.at[0], jnp.where(section == 0, group - 1, group))
    for m in range(1, batches):
        if m > 1:
            first = 1 if m == 2 else 2

            @pl.when(section >= first)
            def _(m=m):
                pl.semaphore_wait(go.at[m - 1], group)

        @pl.when(section > 0)
        def _(m=m):
            send_inputs(0, m)

        @pl.when(section > 0)
        def _(m=m):
            for g in range(1, group):
                side_copy(m, g).wait_recv()
                side_on(m, g).start()

        if m == 1:

            @pl.when(section > 2)
            def _():
                for k in range(batches):
                    send_inputs(1, k)

            spread_targets((2, 1, 0))

        if m == min(2, batches - 1):
            spread_targets((3,))

    def normalize(kind, m, gain_row):
        total = jnp.zeros((seq, cw), jnp.float32)
        for c in range(segs):
            v = act[kind, m, c].astype(jnp.float32)
            total = total + v * v
        mean = jnp.sum(total, axis=-1, keepdims=True) * (1.0 / width)
        scale = lax.rsqrt(mean + epsilon)
        for c in range(segs):
            v = act[kind, m, c].astype(jnp.float32)
            g = gain_row(c)
            nrm[kind, :, c * cw : (c + 1) * cw] = (v * scale * g).astype(jnp.bfloat16)

    def key_gain(c):
        cols = pl.ds(pl.multiple_of(c * cw, cw), cw)
        picked = jnp.where(is_cross, final_gain[:, cols], gains[0:1, cols])
        for p in (1, 3):
            picked = jnp.where(section == p, gains[p : p + 1, cols], picked)
        return picked

    def query_gain(c):
        return gains[2:3, c * cw : (c + 1) * cw]

    def part_copy(m, c, g):
        target = section * group + lax.rem(member + g, group)
        return remote(
            ps.at[m, c],
            pr.at[m, g - 1, c],
            p_send.at[m, g - 1, jnp.where(c < group, 0, 1)],
            p_recv.at[m, g - 1, c],
            target,
        )

    def whole_from(p, m):
        inner = m > 0
        return jnp.logical_and(p < LAYERS - 1, inner)

    def whole(m):
        return whole_from(section, m)

    def part_needed(m, c, g):
        goal = lax.rem(member + g, group)
        return jnp.logical_or(whole(m), lax.rem(c, group) == goal)

    def keeps(m, c):
        return jnp.logical_or(whole(m), lax.rem(c, group) == member)

    def next_copy(m, c, recv):
        return remote(fw.at[m, c], act.at[0, m, c], f_send.at[m], recv, me + group)

    def out_copy(m, c):
        return remote(fw.at[m, c], out.at[m], f_send.at[m], o_recv.at[0], c)

    def prepare(m):
        @pl.when(is_cross)
        def _():
            wait_bytes(act.at[1, m, pl.ds(0, segs - LAYERS)], tgt_rest.at[m])
            normalize(1, m, query_gain)

        @pl.when(m > 0)
        def _():
            wait_bytes(act.at[0, m], later.at[m])
            normalize(0, m, key_gain)

    def project(at, width_at):
        kind = q_src if at < hc else 0
        cols = slice(at, at + width_at)
        qkv[:, cols] = jnp.dot(
            nrm[kind], win[:, cols], preferred_element_type=jnp.float32
        ).astype(jnp.bfloat16)

    def attend(m, pairs):
        length = jnp.where(is_last, tgt_len[m], src_len[m])
        keys = lax.broadcasted_iota(jnp.int32, (2 * seq, seq), 1)
        rows = lax.broadcasted_iota(jnp.int32, (2 * seq, seq), 0)
        rows = jnp.where(rows >= seq, rows - seq, rows)
        bound = jnp.where(is_last, rows, seq)
        allowed = (keys < length) & (keys <= bound)
        lane = lax.broadcasted_iota(jnp.int32, (seq, 2 * HEAD), 1)
        low = lane < HEAD
        for h in pairs:
            at = h * 2 * HEAD
            q2 = qkv[:, at : at + 2 * HEAD]
            k2 = qkv[:, hc + at : hc + at + 2 * HEAD]
            v2 = qkv[:, 2 * hc + at : 2 * hc + at + 2 * HEAD]
            zero = jnp.zeros_like(q2)
            both = jnp.concatenate(
                [jnp.where(low, q2, zero), jnp.where(low, zero, q2)], axis=0
            )
            scores = (
                lax.dot_general(
                    both,
                    k2,
                    (((1,), (1,)), ((), ())),
                    preferred_element_type=jnp.float32,
                )
                * score_scale
            )
            scores = jnp.where(allowed, scores, -1000000000.0)
            top = jnp.max(scores, axis=-1, keepdims=True)
            e = jnp.exp(scores - top)
            weights = (e * (1.0 / jnp.sum(e, axis=-1, keepdims=True))).astype(jnp.bfloat16)
            o = jnp.dot(weights, v2, preferred_element_type=jnp.float32)
            mix[:, at : at + 2 * HEAD] = jnp.where(low, o[:seq], o[seq:]).astype(
                jnp.bfloat16
            )

    def send_parts(m):
        @pl.when(m == 0)
        def _():
            wout_copy.wait()

        def emit(c, carry):
            cols = pl.ds(pl.multiple_of(c * cw, cw), cw)
            part = jnp.dot(mix[...], wout[:, cols], preferred_element_type=jnp.float32)
            own[c] = part
            ps[m, c] = part.astype(jnp.bfloat16)

            @pl.when(jnp.logical_and(c == 0, jnp.logical_or(m > 0, jnp.logical_not(leads))))
            def _():
                pl.semaphore_wait(turn, 1)

            for g in range(1, group):

                @pl.when(part_needed(m, c, g))
                def _():
                    part_copy(m, c, g).start()

            return carry

        lax.fori_loop(0, segs, emit, 0, unroll=True)

    def part_sends(m, at, count, count_half):
        for g in range(1, group):
            sem = p_send.at[m, g - 1, at]

            @pl.when(whole(m))
            def _():
                wait_bytes(ps.at[m, pl.ds(0, count)], sem)

            @pl.when(jnp.logical_not(whole(m)))
            def _():
                wait_bytes(ps.at[m, pl.ds(0, count_half)], sem)

    def hand_over(m):
        @pl.when(jnp.logical_or(m < batches - 1, leads))
        def _():
            pl.semaphore_signal(
                turn, inc=1, device_id={"dp": mate}, device_id_type=MESH
            )

    def combine(m, c):
        @pl.when(keeps(m, c))
        def _():
            total = own[c] + act[q_src, m, c].astype(jnp.float32)
            for g in range(1, group):
                part_copy(m, c, g).wait_recv()
                total = total + pr[m, g - 1, c].astype(jnp.float32)
            fw[m, c] = total.astype(jnp.bfloat16)

            onward = section < LAYERS - 1

            @pl.when(jnp.logical_and(onward, m == 0))
            def _():
                next_copy(m, c, first_own.at[c // group]).start()

            @pl.when(jnp.logical_and(onward, m > 0))
            def _():
                next_copy(m, c, later.at[m]).start()

            @pl.when(jnp.logical_and(is_last, me != c))
            def _():
                out_copy(m, c).start()

            @pl.when(jnp.logical_and(is_last, me == c))
            def _():
                pltpu.make_async_copy(fw.at[m, c], out.at[m], o_recv.at[0]).start()

    head_pairs = hc // (2 * HEAD)
    tile = min(512, hc)

    def add_chunk(c, first):
        v = act[0, 0, c].astype(jnp.float32)
        square = v * v
        own[0] = square if first else own[0] + square
        scaled = (v * key_gain(c)).astype(jnp.bfloat16)
        rows = pl.ds(pl.multiple_of(c * cw, cw), cw)
        for at in range(0, 3 * hc, tile):
            cols = slice(at, at + tile)
            part = jnp.dot(
                scaled, win[rows, cols], preferred_element_type=jnp.float32
            )
            acc[:, cols] = part if first else acc[:, cols] + part

    def start_up():
        @pl.when(section == 0)
        def _():
            for k in range(2, batches):
                send_inputs(0, k)

        win_copy.wait()

        @pl.when(is_cross)
        def _():
            for at in range(0, hc, tile):
                project(at, tile)

        for i in range(LAYERS):
            c = i * group + member

            @pl.when(section > 0)
            def _(i=i, c=c):
                wait_bytes(act.at[0, 0, c], first_own.at[i])
                for g in range(1, group):
                    relay(c, g).start()

            add_chunk(c, i == 0)
        for i in range(LAYERS):
            for g in range(1, group):
                c = i * group + lax.rem(member + g, group)
                wait_bytes(act.at[0, 0, c], first_rest.at[c])
                add_chunk(c, False)
        mean = jnp.sum(own[0], axis=-1, keepdims=True) * (1.0 / width)
        scale = lax.rsqrt(mean + epsilon)

        @pl.when(jnp.logical_not(is_cross))
        def _():
            qkv[:, :hc] = (acc[:, :hc] * scale).astype(jnp.bfloat16)

        qkv[:, hc:] = (acc[:, hc:] * scale).astype(jnp.bfloat16)

    def compute(m):
        @pl.when(m == 0)
        def _():
            start_up()
            attend(m, range(head_pairs))

        @pl.when(m > 0)
        def _():
            for at in range(0, 3 * hc, tile):
                project(at, tile)
            attend(m, range(head_pairs))

    def run(step, m, t):
        kind, i, n = step
        if kind == "turn":
            pl.when(t > 0)(lambda: hand_over(m))
        elif kind == "combine":
            pl.when(t > 0)(lambda: combine(m, i))
        elif kind == "prepare":
            pl.when(t < batches)(lambda: prepare(t))
        else:
            pl.when(t < batches)(lambda: compute(t))

    combines = [("combine", c, segs) for c in range(segs)]
    turn_at = min(TURN, segs - 1)
    steps = combines[:turn_at] + [("turn", 0, 1)] + combines[turn_at:]
    steps += [("prepare", 0, 1), ("compute", 0, 1)]

    def batch_step(t, carry):
        m = t - 1

        @pl.when(t > 0)
        def _():
            send_parts(m)

        for k in range(2, batches):

            @pl.when(jnp.logical_and(section == 0, t == k - 1))
            def _(k=k):
                release(k, 1 if k == 2 else 2)

        for step in steps:
            run(step, m, t)

        return carry

    lax.fori_loop(0, batches + 1, batch_step, 0)

    def forward_sends(m):
        for ahead, count in ((whole(m), segs), (jnp.logical_not(whole(m)), LAYERS)):

            @pl.when(jnp.logical_and(section < LAYERS - 1, ahead))
            def _(count=count):
                wait_bytes(fw.at[m, pl.ds(0, count)], f_send.at[m])

        @pl.when(is_last)
        def _():
            wait_bytes(fw.at[m, pl.ds(0, LAYERS - 1)], f_send.at[m])

    some = pl.ds(0, batches - 1)
    for m in range(batches):
        part_sends(m, 0, group, 1)
        part_sends(m, 1, segs - group, LAYERS - 1)
        forward_sends(m)

    @pl.when(section > 0)
    def _():
        wait_bytes(src, in_send.at[0])
        for g in range(1, group):
            wait_bytes(src.at[some], side_send.at[g - 1])
            wait_bytes(src.at[some], on_send.at[g - 1])

    @pl.when(section == 0)
    def _():
        for g in range(1, group):
            wait_bytes(src.at[some], in_send.at[0])

    @pl.when(jnp.logical_not(is_cross))
    def _():
        wait_bytes(tgt, in_send.at[1])

    for g in range(1, group):
        wait_bytes(act.at[0, 0, pl.ds(0, LAYERS)], r_send.at[g - 1])

        @pl.when(is_cross)
        def _(g=g):
            wait_bytes(tgt, in_send.at[1])
            wait_bytes(act.at[1, :, pl.ds(0, LAYERS - 1)], t_send.at[g - 1])

    wait_bytes(out, o_recv.at[0])


def solution(mesh):
    segs = mesh.shape["segment"]

    def on_device(src, tgt, src_len, tgt_len, w_in, w_out, gains, final_gain):
        batches, seq, cw = src.shape
        group = segs // LAYERS
        w_in, w_out = w_in[0], w_out[0]
        width, qkv_cols = w_in.shape
        hc = w_out.shape[0]
        vmem = pl.BlockSpec(memory_space=pltpu.VMEM)
        smem = pl.BlockSpec(memory_space=pltpu.SMEM)
        anym = pl.BlockSpec(memory_space=pl.ANY)
        bf16 = jnp.bfloat16
        block = (segs, seq, cw)
        dma = pltpu.SemaphoreType.DMA
        return pl.pallas_call(
            functools.partial(kernel, segs),
            out_shape=pltpu.VMEM(src.shape, src.dtype),
            in_specs=[smem, smem, vmem, vmem, anym, anym, vmem, vmem],
            out_specs=vmem,
            scratch_shapes=[
                pltpu.VMEM((width, qkv_cols), bf16),
                pltpu.VMEM((hc, width), bf16),
                pltpu.VMEM((2, batches) + block, bf16),
                pltpu.VMEM((2, seq, width), bf16),
                pltpu.VMEM((seq, qkv_cols), bf16),
                pltpu.VMEM((seq, hc), bf16),
                pltpu.VMEM(block, jnp.float32),
                pltpu.VMEM((batches,) + block, bf16),
                pltpu.VMEM((batches, group - 1) + block, bf16),
                pltpu.VMEM((batches,) + block, bf16),
                pltpu.VMEM((batches - 1, group - 1, seq, cw), bf16),
                pltpu.VMEM((seq, qkv_cols), jnp.float32),
                dma((2,)),
                dma((LAYERS,)),
                dma((segs,)),
                dma((batches,)),
                dma((batches, LAYERS)),
                dma((batches,)),
                dma((2,)),
                dma((batches, group - 1, 2)),
                dma((batches, group - 1, segs)),
                dma((batches,)),
                dma((1,)),
                dma((group - 1,)),
                dma((batches - 1, group - 1)),
                dma((group - 1,)),
                dma((group - 1,)),
                dma((group - 1,)),
                pltpu.SemaphoreType.REGULAR((batches - 1,)),
                pltpu.SemaphoreType.REGULAR,
            ],
            compiler_params=pltpu.CompilerParams(
                collective_id=0,
                has_side_effects=True,
                vmem_limit_bytes=56 * 1024 * 1024,
            ),
        )(src_len, tgt_len, src, tgt, w_in, w_out, gains, final_gain[None])

    return jax.shard_map(
        on_device,
        mesh=mesh,
        in_specs=(
            P("dp", None, "segment"),
            P("dp", None, "segment"),
            P("dp"),
            P("dp"),
            P("segment", None, None),
            P("segment", None, None),
            P(),
            P(),
        ),
        out_specs=P("dp", None, "segment"),
        check_vma=False,
    )
```
